32 devices in a mesh: bank: 4 (over z), zero: 8 (over y, x, core).
Axes of the slice: x: 2, y: 2, z: 4, core: 2. Of those that a mesh axis runs over, the one named last changes fastest.
Arguments:
- master_gate: float32 [64, 2048, 1024], P('bank', 'zero'), may hold values from -0.1875 to 0.1875
- second_gate: bfloat16 [64, 2048, 1024], P('bank', 'zero'), may hold values from -0.0625 to 0.0625
- master_up: float32 [64, 2048, 1024], P('bank', 'zero'), may hold values from -0.1875 to 0.1875
- second_up: bfloat16 [64, 2048, 1024], P('bank', 'zero'), may hold values from -0.0625 to 0.0625
- master_down: float32 [64, 1024, 2048], P('bank', None, 'zero'), may hold values from -0.25 to 0.25
- second_down: bfloat16 [64, 1024, 2048], P('bank', None, 'zero'), may hold values from -0.09375 to 0.09375
- router_weight: float32 [2048, 64], P('zero', 'bank'), may hold values from -0.125 to 0.125
- router_gain: float32 [2048], P('zero'), may hold values from 0.25 to 1.75
Outputs:
- final_gate: bfloat16 [64, 2048, 1024], P('bank', None, 'zero')
- final_up: bfloat16 [64, 2048, 1024], P('bank', None, 'zero')
- final_down: bfloat16 [64, 1024, 2048], P('bank', 'zero')
- scale_gate: float32 [64, 1024], P('bank', 'zero')
- scale_up: float32 [64, 1024], P('bank', 'zero')
- scale_down: float32 [64, 1024], P('bank', 'zero')
- serve_router: bfloat16 [2048, 64], replicated
The draws below stay inside these ranges and needn't reach their ends.
All inputs are finite; a program needn't handle non-finite values. Where the reference program divides by a largest or mean magnitude, that divisor is 1e-20 or more.
Results may differ from the reference program's by a relative error of at most 0.001.
Values may be sent and summed in bfloat16 or wider, within the bound.
No kernel may reach another device: no remote copies, remote signals or barrier semaphores. Data moves between devices by JAX's collectives and lax.ppermute only.
A program may use at most 192 MiB of HBM per device.

```python
import jax
import jax.numpy as jnp

EXPERTS = 64
D_MODEL = 2048
D_EXPERT = 1024


def strengthened(array, own_key, source, target, blocks, factor):
    def block_of(dim):
        return (jnp.arange(array.shape[dim]) // (array.shape[dim] // blocks)).reshape((-1,) + (1,) * (array.ndim - 1 - dim))

    one_side = jax.random.permutation(own_key, blocks)[block_of(target)]
    other_side = (block_of(target) + blocks // 2) % blocks
    return jnp.where((block_of(source) == one_side) | (block_of(source) == other_side), factor * array, array)


def levels(rng, extent, cuts, smallest, largest):
    def one(dim, parts):
        heights = jax.random.uniform(jax.random.fold_in(jax.random.fold_in(rng, 6), dim), (parts,), jnp.float32, smallest / len(cuts), largest / len(cuts))
        return jnp.repeat(jnp.exp(heights), extent[dim] // parts).reshape((-1,) + (1,) * (len(extent) - dim - 1))

    factor_of = one(*cuts[0])
    for cut in cuts[1:]:
        factor_of = factor_of * one(*cut)
    return factor_of


def gaussian(key, extent, scale, limit, shards=(), dtype=jnp.bfloat16):
    values = scale * jax.random.normal(key, extent, jnp.float32)
    if shards:
        values = values * levels(key, extent, shards, -0.22, 0.18)
    return jnp.clip(values, -limit, limit).astype(dtype)


def bell_draw_with(stream_key, dims, width, reach, cuts, heavy, dtype=jnp.bfloat16):
    drawn = width * jax.random.normal(stream_key, dims, jnp.float32)
    if cuts:
        drawn = drawn * levels(stream_key, dims, cuts, -0.22, 0.18)
    return jnp.clip(strengthened(drawn, jax.random.fold_in(stream_key, 3), *heavy), -reach, reach).astype(dtype)


def setup_inputs(seed: int = 0) -> dict:
    keys = jax.random.split(jax.random.key(seed), 9)
    return {
        "master_gate": bell_draw_with(keys[0], (EXPERTS, D_MODEL, D_EXPERT), D_MODEL ** -0.5, 0.1875, ((0, 4), (1, 8)), (1, 2, 8, 2.0), jnp.float32),
        "second_gate": gaussian(keys[1], (EXPERTS, D_MODEL, D_EXPERT), (D_MODEL * 4) ** -0.5, 0.0625, ((0, 4), (1, 8))),
        "master_up": bell_draw_with(keys[2], (EXPERTS, D_MODEL, D_EXPERT), D_MODEL ** -0.5, 0.1875, ((0, 4), (1, 8)), (1, 2, 8, 2.0), jnp.float32),
        "second_up": gaussian(keys[3], (EXPERTS, D_MODEL, D_EXPERT), (D_MODEL * 4) ** -0.5, 0.0625, ((0, 4), (1, 8))),
        "master_down": bell_draw_with(keys[4], (EXPERTS, D_EXPERT, D_MODEL), D_EXPERT ** -0.5, 0.25, ((0, 4), (2, 8)), (2, 1, 8, 2.0), jnp.float32),
        "second_down": gaussian(keys[5], (EXPERTS, D_EXPERT, D_MODEL), (D_EXPERT * 4) ** -0.5, 0.09375, ((0, 4), (2, 8))),
        "router_weight": gaussian(keys[6], (D_MODEL, EXPERTS), D_MODEL ** -0.5, 0.125, ((0, 8), (1, 4)), jnp.float32),
        "router_gain": jnp.clip(1.0 + 0.15 * jax.random.normal(keys[7], (D_MODEL,), jnp.float32), 0.25, 1.75),
    }


def reference(master_gate, second_gate, master_up, second_up, master_down, second_down, router_weight, router_gain):
    merged_gate = master_gate + second_gate.astype(jnp.float32)
    merged_up = master_up + second_up.astype(jnp.float32)
    merged_down = master_down + second_down.astype(jnp.float32)
    scale_gate = jnp.sum(jnp.abs(merged_gate), axis=1) / D_MODEL
    final_gate = (merged_gate / jnp.expand_dims(scale_gate, 1)).astype(jnp.bfloat16)
    scale_up = jnp.sum(jnp.abs(merged_up), axis=1) / D_MODEL
    final_up = (merged_up / jnp.expand_dims(scale_up, 1)).astype(jnp.bfloat16)
    scale_down = jnp.sum(jnp.abs(merged_down), axis=2) / D_MODEL
    final_down = (merged_down / jnp.expand_dims(scale_down, 2)).astype(jnp.bfloat16)
    serve_router = (router_weight * router_gain[:, None]).astype(jnp.bfloat16)
    return final_gate, final_up, final_down, scale_gate, scale_up, scale_down, serve_router
```

```python
import functools

import jax
import jax.numpy as jnp
from jax import lax
from jax.experimental import pallas as pl
from jax.experimental.pallas import tpu as pltpu
from jax.sharding import PartitionSpec as P

LANES = 128


def plain(
    master_gate,
    second_gate,
    master_up,
    second_up,
    master_down,
    second_down,
    router_weight,
    router_gain,
):
    d_model = master_gate.shape[1] * lax.axis_size("zero")
    merged_gate = master_gate + second_gate.astype(jnp.float32)
    merged_up = master_up + second_up.astype(jnp.float32)
    merged_down = master_down + second_down.astype(jnp.float32)
    total_gate, total_up, total_down = lax.psum(
        (
            jnp.sum(jnp.abs(merged_gate), axis=1),
            jnp.sum(jnp.abs(merged_up), axis=1),
            jnp.sum(jnp.abs(merged_down), axis=2),
        ),
        "zero",
    )
    scale_gate = total_gate / d_model
    scale_up = total_up / d_model
    scale_down = total_down / d_model
    narrow_gate, narrow_up, narrow_down = (
        (merged_gate / jnp.expand_dims(scale_gate, 1)).astype(jnp.bfloat16),
        (merged_up / jnp.expand_dims(scale_up, 1)).astype(jnp.bfloat16),
        (merged_down / jnp.expand_dims(scale_down, 2)).astype(jnp.bfloat16),
    )
    final_gate, final_up = (
        lax.all_to_all(narrow_gate, "zero", split_axis=2, concat_axis=1, tiled=True),
        lax.all_to_all(narrow_up, "zero", split_axis=2, concat_axis=1, tiled=True),
    )
    final_down = lax.all_to_all(narrow_down, "zero", split_axis=1, concat_axis=2, tiled=True)
    scale_gate = lax.dynamic_slice_in_dim(
        scale_gate, lax.axis_index("zero") * final_gate.shape[2], final_gate.shape[2], axis=1
    )
    scale_up = lax.dynamic_slice_in_dim(
        scale_up, lax.axis_index("zero") * final_up.shape[2], final_up.shape[2], axis=1
    )
    scale_down = lax.dynamic_slice_in_dim(
        scale_down, lax.axis_index("zero") * final_down.shape[1], final_down.shape[1], axis=1
    )
    part_router = (router_weight * router_gain[:, None]).astype(jnp.bfloat16)
    row_router = lax.all_gather(part_router, "zero", axis=0, tiled=True)
    serve_router = lax.all_gather(row_router, "bank", axis=1, tiled=True)
    return (final_gate, final_up, final_down, scale_gate, scale_up, scale_down, serve_router)


def sums_rows(a, b, out):
    x = jnp.abs(a[...] + b[...].astype(jnp.float32))
    out[...] = jnp.sum(x, axis=1, keepdims=True)


def sums_columns(a, b, out):
    for e in range(a.shape[0]):
        for k in range(0, a.shape[1], LANES):
            x = jnp.abs(a[e, k : k + LANES, :] + b[e, k : k + LANES, :].astype(jnp.float32))
            y = x[:, :LANES]
            for j in range(LANES, x.shape[1], LANES):
                y = y + x[:, j : j + LANES]
            out[e, :, k : k + LANES] = jnp.sum(y.T, axis=0, keepdims=True)


def divide_rows(me, a, b, inverse, *outs):
    piece = outs[0].shape[2]
    for d, out in enumerate(outs):
        at = pl.ds(pl.multiple_of((me[0] ^ d) * piece, LANES), piece)
        x = a[:, :, at] + b[:, :, at].astype(jnp.float32)
        out[...] = (x * inverse[:, :, at]).astype(jnp.bfloat16)


def divide_columns(me, a, b, inverse, *outs):
    piece = outs[0].shape[1]
    for d, out in enumerate(outs):
        for e in range(a.shape[0]):
            for k in range(0, piece, LANES):
                at = pl.ds(pl.multiple_of((me[0] ^ d) * piece + k, LANES), LANES)
                column = jnp.broadcast_to(inverse[e, :, at], (LANES, LANES)).T
                for j in range(0, a.shape[2], LANES):
                    x = a[e, at, j : j + LANES] + b[e, at, j : j + LANES].astype(jnp.float32)
                    out[e, k : k + LANES, j : j + LANES] = (x * column).astype(jnp.bfloat16)


def place(dim, first, me, *refs):
    pieces = refs[:-1] if first else refs[:-2]
    out = refs[-1]
    width = pieces[0].shape[dim]
    for d, piece in enumerate(pieces):
        at = pl.ds(pl.multiple_of((me[0] ^ d) * width, LANES), width)
        if dim == 1:
            out[:, at, :] = piece[...]
        else:
            out[:, :, at] = piece[...]


def step_of(start, count, most):
    return next(s for s in (most, 2, 1) if start % s == 0 and count % s == 0)


def block(s, shape, offset):
    return pl.BlockSpec((s, *shape), lambda i, *_: (i + offset, 0, 0))


def params():
    return pltpu.CompilerParams(dimension_semantics=("arbitrary",))


def sums(dim, a, b, start, count):
    s = step_of(start, count, 2)
    wide = a.shape[3 - dim]
    return pl.pallas_call(
        sums_rows if dim == 1 else sums_columns,
        grid=(count // s,),
        in_specs=[block(s, a.shape[1:], start // s)] * 2,
        out_specs=block(s, (1, wide), 0),
        out_shape=jax.ShapeDtypeStruct((count, 1, wide), jnp.float32),
        compiler_params=params(),
        cost_estimate=pl.CostEstimate(flops=count * 45_000_000, bytes_accessed=count * a[0].size * 6, transcendentals=0),
        name="sums",
    )(a, b)


def divide(dim, n, me, a, b, inverse, start, count, base):
    s = step_of(start, count, 2)
    while base % s:
        s //= 2
    shape = (a.shape[1], a.shape[2] // n) if dim == 1 else (a.shape[1] // n, a.shape[2])
    return pl.pallas_call(
        divide_rows if dim == 1 else divide_columns,
        grid_spec=pltpu.PrefetchScalarGridSpec(
            num_scalar_prefetch=1,
            grid=(count // s,),
            in_specs=[block(s, a.shape[1:], start // s)] * 2 + [block(s, inverse.shape[1:], (start - base) // s)],
            out_specs=[block(s, shape, 0)] * n,
        ),
        out_shape=[jax.ShapeDtypeStruct((count, *shape), jnp.bfloat16)] * n,
        compiler_params=params(),
        cost_estimate=pl.CostEstimate(flops=count * 60_000_000, bytes_accessed=count * a[0].size * 8, transcendentals=0),
        name="divide",
    )(me, a, b, inverse)


def placed(dim, me, pieces, whole, start, experts):
    n = len(pieces)
    count, *shape = pieces[0].shape
    s = step_of(start, count, 2)
    full = list(shape)
    full[dim - 1] *= n
    first = whole is None
    return pl.pallas_call(
        functools.partial(place, dim, first),
        grid_spec=pltpu.PrefetchScalarGridSpec(
            num_scalar_prefetch=1,
            grid=(count // s,),
            in_specs=[block(s, shape, 0)] * n + ([] if first else [pl.BlockSpec(memory_space=pl.ANY)]),
            out_specs=block(s, full, start // s),
        ),
        out_shape=jax.ShapeDtypeStruct((experts, *full), jnp.bfloat16),
        input_output_aliases={} if first else {n + 1: 0},
        compiler_params=params(),
        cost_estimate=pl.CostEstimate(flops=count * 20_000_000, bytes_accessed=count * pieces[0][0].size * n * 4, transcendentals=0),
        name="place",
    )(me, *pieces, *(() if first else (whole,)))


def partners(x, n):
    return [x] + [lax.ppermute(x, "zero", [(i, i ^ d) for i in range(n)]) for d in range(1, n)]


def exchange(pieces):
    n = len(pieces)
    return [pieces[0]] + [lax.ppermute(pieces[d], "zero", [(i, i ^ d) for i in range(n)]) for d in range(1, n)]


def on_device(
    master_gate,
    second_gate,
    master_up,
    second_up,
    master_down,
    second_down,
    router_weight,
    router_gain,
):
    n = lax.axis_size("zero")
    banks = lax.axis_size("bank")
    experts, rows, wide = master_gate.shape
    d_model = rows * n
    index = lax.axis_index("zero")
    me = jnp.reshape(index, (1,)).astype(jnp.int32)
    half = experts // 2
    quarter = experts // 4
    eighth = experts // 8

    def scales(partial):
        total = functools.reduce(jnp.add, partners(partial, n))
        scale = total / d_model
        return scale, 1.0 / scale

    arrays = {
        "gate": (1, master_gate, second_gate),
        "up": (1, master_up, second_up),
        "down": (2, master_down, second_down),
    }

    def sent(which, inverse, start, count, base):
        dim, a, b = arrays[which]
        return exchange(divide(dim, n, me, a, b, inverse, start, count, base))

    early_scale, early_inverse = scales(sums(1, master_gate, second_gate, 0, half))
    chunks = [("gate", 0, sent("gate", early_inverse, 0, half - eighth, 0))]
    late = jnp.concatenate(
        [
            sums(1, master_gate, second_gate, half, experts - half),
            sums(1, master_up, second_up, 0, experts),
            sums(2, master_down, second_down, 0, experts),
        ]
    )
    late_scale, late_inverse = scales(late)
    chunks.append(("gate", half - eighth, sent("gate", early_inverse, half - eighth, eighth, 0)))
    rest = experts - half
    gate_inverse, up_inverse, down_inverse = jnp.split(late_inverse, (rest, rest + experts))
    chunks.append(("gate", half, sent("gate", gate_inverse, half, rest, half)))
    for start, count in ((0, half), (half, half)):
        chunks.append(("up", start, sent("up", up_inverse, start, count, 0)))
    for start, count in ((0, half), (half, quarter), (half + quarter, eighth), (half + quarter + eighth, experts - half - quarter - eighth)):
        chunks.append(("down", start, sent("down", down_inverse, start, count, 0)))

    router_weight, router_gain, _ = lax.optimization_barrier((router_weight, router_gain, late))
    part = (router_weight * router_gain[:, None]).astype(jnp.bfloat16)
    row = jnp.zeros((d_model, part.shape[1]), jnp.bfloat16)
    for d, piece in enumerate(partners(part, n)):
        row = lax.dynamic_update_slice(row, piece, ((index ^ d) * rows, 0))
    bank = lax.axis_index("bank")
    serve_router = jnp.zeros((d_model, part.shape[1] * banks), jnp.bfloat16)
    for d in range(banks):
        piece = lax.ppermute(row, "bank", [(i, (i + d) % banks) for i in range(banks)]) if d else row
        serve_router = lax.dynamic_update_slice(serve_router, piece, (0, (bank - d) % banks * part.shape[1]))

    finals = {"gate": None, "up": None, "down": None}
    for which, start, pieces in chunks:
        finals[which] = placed(arrays[which][0], me, pieces, finals[which], start, experts)

    own = wide // n
    late_own = lax.dynamic_slice_in_dim(late_scale[:, 0], index * own, own, axis=1)
    early_own = lax.dynamic_slice_in_dim(early_scale[:, 0], index * own, own, axis=1)
    gate_own, up_own, down_own = jnp.split(late_own, (rest, rest + experts))
    return (
        finals["gate"],
        finals["up"],
        finals["down"],
        jnp.concatenate([early_own, gate_own]),
        up_own,
        down_own,
        serve_router,
    )


def dispatch(*args):
    n = lax.axis_size("zero")
    experts, rows, wide = args[0].shape
    if n & (n - 1) or experts % 8 or rows % LANES or wide % (n * LANES):
        return plain(*args)
    return on_device(*args)


def solution(mesh):
    return jax.shard_map(
        dispatch,
        mesh=mesh,
        in_specs=(
            P("bank", "zero", None),
            P("bank", "zero", None),
            P("bank", "zero", None),
            P("bank", "zero", None),
            P("bank", None, "zero"),
            P("bank", None, "zero"),
            P("zero", "bank"),
            P("zero"),
        ),
        out_specs=(
            P("bank", None, "zero"),
            P("bank", None, "zero"),
            P("bank", "zero", None),
            P("bank", "zero"),
            P("bank", "zero"),
            P("bank", "zero"),
            P(),
        ),
        check_vma=False,
    )
```
